32 devices in a mesh: seq: 2 (over x), mp: 4 (over y, core), dp: 4 (over z).
Axes of the slice: x: 2, y: 2, z: 4, core: 2. Of those that a mesh axis runs over, the one named last changes fastest.
Arguments:
- tokens: bfloat16 [16384, 2048], P(('dp', 'seq'), 'mp'), parts along dimension 0, may hold values from -6 to 6
- w_query: bfloat16 [2048, 2048], P(None, 'mp'), may hold values from -0.125 to 0.125
- w_key: bfloat16 [2048, 2048], P(None, 'mp'), may hold values from -0.125 to 0.125
- w_value: bfloat16 [2048, 2048], P(None, 'mp'), may hold values from -0.125 to 0.125
- w_gate: bfloat16 [2048, 2048], P(None, 'mp'), may hold values from -0.125 to 0.125
- decay_exponent: int32 [16], P('mp'), may hold values from 5 to 16
- forget: float32 [16384, 16], P(('dp', 'seq'), 'mp'), parts along dimension 0, may hold values from 0 to 0.69
- norm_gain: float32 [2048], replicated, may hold values from 0.1 to 1.9
Outputs:
- retained: bfloat16 [16384, 2048], P(('dp', 'seq', 'mp')), parts along dimension 0
The draws below stay inside these ranges and needn't reach their ends.
There are 4 independent parts, one for each index of `dp`. The reference program is written for one: setup_inputs(seed, part) draws one part's arguments, and reference() takes and returns one part's arrays. A program takes and returns all parts, laid end to end along the dimension named above; an argument that names none is the same for every part. Nothing has to cross between parts.
All inputs are finite; a program needn't handle non-finite values.
Results may differ from the reference program's by a relative error of at most 0.015.
Values may be sent and summed in bfloat16 or wider, within the bound.
No kernel may reach another device: no remote copies, remote signals or barrier semaphores. Data moves between devices by JAX's collectives and lax.ppermute only.
A program may use at most 64 MiB of HBM per device.

```python
import jax
import jax.numpy as jnp
from jax import lax

D = 2048
HEADS = 16
DH = 128
TOKENS = 4096
FEATURES = 2048


def draw_forget(key, part):
    first_key, second_key = jax.random.split(jax.random.fold_in(key, 11))
    chance = jax.random.uniform(first_key, (TOKENS, HEADS), jnp.float32)
    amount = jax.random.uniform(second_key, (TOKENS, HEADS), jnp.float32, 0.22, 0.69)
    return jnp.where(chance < 6.0 / TOKENS, amount, 0.0).astype(jnp.float32)


def with_ends(entries, key, low, high):
    spot = [jax.random.randint(jax.random.fold_in(key, axis), (), 0, length) for axis, length in enumerate(entries.shape)]
    longest = entries.shape.index(max(entries.shape))
    next_to = spot[:longest] + [(spot[longest] + 1) % entries.shape[longest]] + spot[longest + 1:]
    return entries.at[tuple(spot)].set(low).at[tuple(next_to)].set(high)


def level_of(rng, extent, shards, smallest, top_value):
    level, own = 1.0, jax.random.fold_in(rng, 6)
    for axis_at, shards_of in shards:
        heights = jnp.exp(jax.random.uniform(jax.random.fold_in(own, axis_at), (shards_of,), jnp.float32, smallest / len(shards), top_value / len(shards)))
        level = level * jnp.repeat(heights, extent[axis_at] // shards_of).reshape([-1 if axis == axis_at else 1 for axis in range(len(extent))])
    return level


def normal_values(key, extent, spread, reach, shards=(), kind=jnp.bfloat16):
    level = level_of(key, extent, shards, -0.22, 0.18) if shards else 1.0
    values = jax.random.normal(key, extent, jnp.float32) * spread * level
    return jnp.minimum(jnp.maximum(values, -reach), reach).astype(kind)


def setup_inputs(seed: int = 0, part: int = 0) -> dict:
    keys = jax.random.split(jax.random.key(seed), 9)
    part_splits = jax.random.split(jax.random.fold_in(keys[8], part), 9)
    return {
        "tokens": normal_values(part_splits[0], (TOKENS, D), 1.0, 6.0, ((0, 2), (1, 4))),
        "w_query": normal_values(keys[1], (D, FEATURES), D ** -0.5, 0.125, ((1, 4),)),
        "w_key": normal_values(keys[2], (D, FEATURES), D ** -0.5, 0.125, ((1, 4),)),
        "w_value": normal_values(keys[3], (D, FEATURES), D ** -0.5, 0.125, ((1, 4),)),
        "w_gate": normal_values(keys[4], (D, FEATURES), D ** -0.5, 0.125, ((1, 4),)),
        "decay_exponent": with_ends(jax.random.randint(keys[5], (HEADS,), 5, 17), jax.random.fold_in(keys[5], 1), 5, 16).astype(jnp.int32),
        "forget": draw_forget(jax.random.fold_in(jax.random.fold_in(keys[8], part), 71), part),
        "norm_gain": jnp.clip(1.0 + 0.18 * jax.random.normal(keys[7], (FEATURES,), jnp.float32), 0.1, 1.9),
    }


def retention(queries, key_rows, values, logdecay):
    seq_rows = queries.shape[0]
    head_count = logdecay.shape[1]
    head_width = queries.shape[1] // head_count
    block_rows = 512 if seq_rows % 512 == 0 else seq_rows
    block_count = seq_rows // block_rows

    def shaped(source):
        return source.reshape(block_count, block_rows, head_count, head_width)
    decays = logdecay.reshape(block_count, block_rows, head_count)
    position = lax.broadcasted_iota(jnp.int32, (block_rows, block_rows), 0)
    earlier = lax.broadcasted_iota(jnp.int32, (block_rows, block_rows), 1)
    causal = position >= earlier

    def advance(kv_state, pieces):
        query_blk, key_blk, value_blk, decay_blk = pieces
        running = jnp.cumsum(decay_blk, axis=0)
        heads_first = running.T
        log_gap = heads_first[:, :, None] - heads_first[:, None, :]
        decay_mask = jnp.where(causal[None], jnp.exp(jnp.where(causal[None], log_gap, 0.0)), 0.0)
        query_float = query_blk.astype(jnp.float32)
        key_float = key_blk.astype(jnp.float32)
        value_float = value_blk.astype(jnp.float32)
        scores = (jnp.einsum('tha,sha->hts', query_float, key_float) * decay_mask).astype(jnp.bfloat16)
        inner = jnp.einsum('hts,shb->thb', scores.astype(jnp.float32), value_float)
        carried = jnp.einsum('tha,hab->thb', query_float * jnp.exp(running)[:, :, None], kv_state, precision=lax.Precision.HIGHEST)
        key_scaled = key_float * jnp.exp(running[-1:] - running)[:, :, None]
        kv_state = jnp.exp(running[-1])[:, None, None] * kv_state + jnp.einsum('sha,shb->hab', key_scaled, value_float, precision=lax.Precision.HIGHEST)
        return (kv_state, (inner + carried).astype(jnp.bfloat16))
    initial = jnp.zeros((head_count, head_width, head_width), jnp.float32)
    final_state, outputs = lax.scan(advance, initial, (shaped(queries), shaped(key_rows), shaped(values), decays))
    return outputs.reshape(seq_rows, head_count * head_width)

def reference(tokens, w_query, w_key, w_value, w_gate, decay_exponent, forget, norm_gain):
    queries = jnp.dot(tokens, w_query, preferred_element_type=jnp.float32).astype(jnp.bfloat16)
    key_rows = (jnp.dot(tokens, w_key, preferred_element_type=jnp.float32) * DH ** (-0.5)).astype(jnp.bfloat16)
    values = jnp.dot(tokens, w_value, preferred_element_type=jnp.float32).astype(jnp.bfloat16)
    gate = jnp.dot(tokens, w_gate, preferred_element_type=jnp.float32).astype(jnp.bfloat16)
    rate = jnp.log1p(-jnp.exp2(-decay_exponent.astype(jnp.float32)))
    logdecay = rate[None, :] - forget
    output = retention(queries, key_rows, values, logdecay).astype(jnp.float32)
    squares = lax.optimization_barrier(jnp.mean(output * output, axis=1))
    rstd = lax.rsqrt(squares + 1e-06)
    gated = jax.nn.silu(gate.astype(jnp.float32)) * output * rstd[:, None] * norm_gain[None, :]
    return gated.astype(jnp.bfloat16)
```

```python
import functools

import jax
import jax.numpy as jnp
from jax import lax
from jax.experimental import pallas as pl
from jax.experimental.pallas import tpu as pltpu
from jax.sharding import PartitionSpec as P

DH = 128


def block_of(rows, most):
    block = min(rows, most)
    while rows % block:
        block //= 2
    return block


def running_sum(decay_rows):
    width = decay_rows.shape[1]
    upto = (
        lax.broadcasted_iota(jnp.int32, (width, width), 0)
        <= lax.broadcasted_iota(jnp.int32, (width, width), 1)
    ).astype(jnp.float32)
    return jnp.dot(
        decay_rows, upto, precision=lax.Precision.HIGHEST, preferred_element_type=jnp.float32
    )


def next_state(state, key_blk, value_blk, column, last):
    scaled = (key_blk.astype(jnp.float32) * jnp.exp(last - column)).astype(jnp.bfloat16)
    return jnp.exp(last) * state + lax.dot_general(
        scaled, value_blk, (((0,), (0,)), ((), ())), preferred_element_type=jnp.float32
    )


def state_kernel(decay_ref, key_ref, value_ref, state_ref, total_ref, *, heads, width):
    @pl.when(pl.program_id(0) == 0)
    def _():
        state_ref[...] = jnp.zeros_like(state_ref)
        total_ref[...] = jnp.zeros_like(total_ref)

    running = running_sum(decay_ref[...])
    columns = running.T
    last_at = running.shape[1] - 1
    for h in range(heads):
        at = slice(h * width, (h + 1) * width)
        last = running[h : h + 1, last_at:]
        state_ref[h] = next_state(
            state_ref[h], key_ref[:, at], value_ref[:, at], columns[:, h : h + 1], last
        )
    total_ref[...] += jnp.broadcast_to(running[:, last_at:], total_ref.shape)


def retain_kernel(
    decay_ref, query_ref, key_ref, value_ref, initial_ref, out_ref, state_ref, *, heads, width
):
    @pl.when(pl.program_id(0) == 0)
    def _():
        state_ref[...] = initial_ref[...]

    running = running_sum(decay_ref[...])
    columns = running.T
    size = running.shape[1]
    causal = lax.broadcasted_iota(jnp.int32, (size, size), 0) >= lax.broadcasted_iota(
        jnp.int32, (size, size), 1
    )
    for h in range(heads):
        at = slice(h * width, (h + 1) * width)
        row = running[h : h + 1, :]
        column = columns[:, h : h + 1]
        last = running[h : h + 1, size - 1 :]
        query = query_ref[:, at]
        key_blk = key_ref[:, at]
        value_blk = value_ref[:, at]
        mask = jnp.where(causal, jnp.exp(column - row), 0.0)
        scores = lax.dot_general(
            query, key_blk, (((1,), (1,)), ((), ())), preferred_element_type=jnp.float32
        )
        scores = (scores * mask).astype(jnp.bfloat16)
        state = state_ref[h]
        inner = jnp.dot(scores, value_blk, preferred_element_type=jnp.float32)
        carried = jnp.dot(query, state.astype(jnp.bfloat16), preferred_element_type=jnp.float32)
        out_ref[:, at] = (inner + jnp.exp(column) * carried).astype(jnp.bfloat16)
        state_ref[h] = next_state(state, key_blk, value_blk, column, last)


def norm_kernel(out_ref, gate_ref, gain_ref, result_ref):
    groups, _, width = out_ref.shape
    outs = [out_ref[g].astype(jnp.float32) for g in range(groups)]
    squares = sum(jnp.sum(o * o, axis=1, keepdims=True) for o in outs)
    rstd = lax.rsqrt(squares / (groups * width) + 1e-06)
    for g in range(groups):
        at = slice(g * width, (g + 1) * width)
        gate = gate_ref[g].astype(jnp.float32)
        silu = gate * (1.0 / (1.0 + jnp.exp(-gate)))
        result_ref[:, at] = (silu * outs[g] * rstd * gain_ref[:, at]).astype(jnp.bfloat16)


def local_state(decay_rows, key_rows, values, heads, width):
    rows, local = key_rows.shape
    block = block_of(rows, 256)
    return pl.pallas_call(
        functools.partial(state_kernel, heads=heads, width=width),
        grid=(rows // block,),
        in_specs=[
            pl.BlockSpec((heads, block), lambda i: (0, i)),
            pl.BlockSpec((block, local), lambda i: (i, 0)),
            pl.BlockSpec((block, local), lambda i: (i, 0)),
        ],
        out_specs=[
            pl.BlockSpec((heads, width, width), lambda i: (0, 0, 0)),
            pl.BlockSpec((heads, 128), lambda i: (0, 0)),
        ],
        out_shape=[
            jax.ShapeDtypeStruct((heads, width, width), jnp.float32),
            jax.ShapeDtypeStruct((heads, 128), jnp.float32),
        ],
        name="local_state",
    )(decay_rows, key_rows, values)


def retain(decay_rows, queries, key_rows, values, initial, heads, width):
    rows, local = key_rows.shape
    block = block_of(rows, 256)
    token_spec = pl.BlockSpec((block, local), lambda i: (i, 0))
    return pl.pallas_call(
        functools.partial(retain_kernel, heads=heads, width=width),
        grid=(rows // block,),
        in_specs=[
            pl.BlockSpec((heads, block), lambda i: (0, i)),
            token_spec,
            token_spec,
            token_spec,
            pl.BlockSpec((heads, width, width), lambda i: (0, 0, 0)),
        ],
        out_specs=token_spec,
        out_shape=jax.ShapeDtypeStruct((rows, local), jnp.bfloat16),
        scratch_shapes=[pltpu.VMEM((heads, width, width), jnp.float32)],
        name="retain",
    )(decay_rows, queries, key_rows, values, initial)


def gated_norm(output, gate, gain):
    groups, rows, width = output.shape
    block = block_of(rows, 128)
    piece = pl.BlockSpec((groups, block, width), lambda i: (0, i, 0))
    return pl.pallas_call(
        norm_kernel,
        grid=(rows // block,),
        in_specs=[piece, piece, pl.BlockSpec((1, groups * width), lambda i: (0, 0))],
        out_specs=pl.BlockSpec((block, groups * width), lambda i: (i, 0)),
        out_shape=jax.ShapeDtypeStruct((rows, groups * width), jnp.bfloat16),
        name="gated_norm",
    )(output, gate, gain.reshape(1, -1))


def carried_in(state, total, axis, count):
    decay = jnp.exp(total[:, 0])
    sent = state.astype(jnp.bfloat16)
    incoming = None
    for hop in range(count - 1, 0, -1):
        moves = [(i, i + hop) for i in range(count - hop)]
        arrived = lax.ppermute(sent, axis, moves).astype(jnp.float32)
        if incoming is not None:
            factor = lax.ppermute(decay, axis, moves)
            arrived = arrived + factor[:, None, None] * incoming
        incoming = arrived
    return jnp.zeros_like(state) if incoming is None else incoming


def body(seq_count, mp_count, tokens, w_query, w_key, w_value, w_gate, decay_exponent, forget, norm_gain):
    seq_rows = tokens.shape[0]
    local_width = w_query.shape[1]
    heads = decay_exponent.shape[0]
    width = local_width // heads
    piece = lax.all_gather(tokens, "mp", axis=1, tiled=True)
    rate = jnp.log1p(-jnp.exp2(-decay_exponent.astype(jnp.float32)))
    decay_rows = rate[:, None] - forget.T

    def project(weight):
        return jnp.dot(piece, weight, preferred_element_type=jnp.float32)

    def exchange(source):
        pieces = source.reshape(mp_count, seq_rows // mp_count, local_width)
        return lax.all_to_all(pieces, "mp", split_axis=0, concat_axis=0, tiled=True)

    gate = project(w_gate).astype(jnp.bfloat16)
    moved_gate = exchange(gate)
    key_rows = (project(w_key) * DH ** (-0.5)).astype(jnp.bfloat16)
    values = project(w_value).astype(jnp.bfloat16)
    state, total = local_state(decay_rows, key_rows, values, heads, width)
    incoming = carried_in(state, total, "seq", seq_count)
    queries = project(w_query).astype(jnp.bfloat16)
    output = retain(decay_rows, queries, key_rows, values, incoming, heads, width)
    moved_output = exchange(output)
    return gated_norm(moved_output, moved_gate, norm_gain)


def solution(mesh):
    placed = (
        P(("dp", "seq"), "mp"),
        P(None, "mp"),
        P(None, "mp"),
        P(None, "mp"),
        P(None, "mp"),
        P("mp"),
        P(("dp", "seq"), "mp"),
        P(),
    )
    return jax.shard_map(
        functools.partial(body, mesh.shape["seq"], mesh.shape["mp"]),
        mesh=mesh,
        in_specs=placed,
        out_specs=P(("dp", "seq", "mp"), None),
        check_vma=False,
    )
```

```python
import functools

import jax
import jax.numpy as jnp
from jax import lax
from jax.experimental import pallas as pl
from jax.experimental.pallas import tpu as pltpu
from jax.sharding import PartitionSpec as P

DH = 128
CHUNKS = 4


def block_of(rows, most):
    block = min(rows, most)
    while rows % block:
        block //= 2
    return block


def running_sum(decay_rows):
    width = decay_rows.shape[1]
    upto = (
        lax.broadcasted_iota(jnp.int32, (width, width), 0)
        <= lax.broadcasted_iota(jnp.int32, (width, width), 1)
    ).astype(jnp.float32)
    return jnp.dot(
        decay_rows, upto, precision=lax.Precision.HIGHEST, preferred_element_type=jnp.float32
    )


def next_state(state, key_blk, value_blk, column, last):
    scaled = (key_blk.astype(jnp.float32) * jnp.exp(last - column)).astype(jnp.bfloat16)
    return jnp.exp(last) * state + lax.dot_general(
        scaled, value_blk, (((0,), (0,)), ((), ())), preferred_element_type=jnp.float32
    )


def project_kernel(order_ref, decay_ref, *refs, pieces, heads, width, aliased):
    parts = refs[:pieces]
    weights = refs[pieces : pieces + 4]
    before_ref, total_before_ref = refs[pieces + 4 : pieces + 6]
    outs = refs[pieces + 6 + (4 if aliased else 0) :]
    gate_ref, key_ref, value_ref, query_ref, state_ref, total_ref = outs

    @pl.when(pl.program_id(0) == 0)
    def _():
        state_ref[...] = before_ref[...]
        total_ref[...] = total_before_ref[...]

    depth = parts[0].shape[1]

    def project(weight):
        acc = None
        for p in range(pieces):
            start = pl.multiple_of(order_ref[p] * depth, depth)
            one = jnp.dot(
                parts[p][...],
                weight[pl.ds(start, depth), :],
                preferred_element_type=jnp.float32,
            )
            acc = one if acc is None else acc + one
        return acc

    key_ref[...] = (project(weights[1]) * DH ** (-0.5)).astype(jnp.bfloat16)
    value_ref[...] = project(weights[2]).astype(jnp.bfloat16)
    gate_ref[...] = project(weights[0]).astype(jnp.bfloat16)
    query_ref[...] = project(weights[3]).astype(jnp.bfloat16)
    running = running_sum(decay_ref[...])
    columns = running.T
    last_at = running.shape[1] - 1
    for h in range(heads):
        at = slice(h * width, (h + 1) * width)
        last = running[h : h + 1, last_at:]
        state_ref[h] = next_state(
            state_ref[h], key_ref[:, at], value_ref[:, at], columns[:, h : h + 1], last
        )
    total_ref[...] += jnp.broadcast_to(running[:, last_at:], total_ref.shape)


def retain_kernel(
    decay_ref, query_ref, key_ref, value_ref, initial_ref, out_ref, state_ref, *, heads, width
):
    @pl.when(pl.program_id(0) == 0)
    def _():
        state_ref[...] = initial_ref[...]

    running = running_sum(decay_ref[...])
    columns = running.T
    size = running.shape[1]
    causal = lax.broadcasted_iota(jnp.int32, (size, size), 0) >= lax.broadcasted_iota(
        jnp.int32, (size, size), 1
    )
    for h in range(heads):
        at = slice(h * width, (h + 1) * width)
        row = running[h : h + 1, :]
        column = columns[:, h : h + 1]
        last = running[h : h + 1, size - 1 :]
        query = query_ref[:, at]
        key_blk = key_ref[:, at]
        value_blk = value_ref[:, at]
        mask = jnp.where(causal, jnp.exp(column - row), 0.0)
        scores = lax.dot_general(
            query, key_blk, (((1,), (1,)), ((), ())), preferred_element_type=jnp.float32
        )
        scores = (scores * mask).astype(jnp.bfloat16)
        state = state_ref[h]
        inner = jnp.dot(scores, value_blk, preferred_element_type=jnp.float32)
        carried = jnp.dot(query, state.astype(jnp.bfloat16), preferred_element_type=jnp.float32)
        out_ref[:, at] = (inner + jnp.exp(column) * carried).astype(jnp.bfloat16)
        state_ref[h] = next_state(state, key_blk, value_blk, column, last)


def norm_kernel(out_ref, gate_ref, gain_ref, result_ref):
    groups, _, width = out_ref.shape
    outs = [out_ref[g].astype(jnp.float32) for g in range(groups)]
    squares = sum(jnp.sum(o * o, axis=1, keepdims=True) for o in outs)
    rstd = lax.rsqrt(squares / (groups * width) + 1e-06)
    for g in range(groups):
        at = slice(g * width, (g + 1) * width)
        gate = gate_ref[g].astype(jnp.float32)
        silu = gate * (1.0 / (1.0 + jnp.exp(-gate)))
        result_ref[:, at] = (silu * outs[g] * rstd * gain_ref[:, at]).astype(jnp.bfloat16)


def project_chunk(order, decay_rows, parts, weights, before, total, buffers, first, rows, heads, width):
    chunk_rows, depth = parts[0].shape
    full, local = weights[0].shape
    block = block_of(chunk_rows, 256)
    skip = first // block
    part_spec = pl.BlockSpec((block, depth), lambda i, o: (i, 0))
    weight_spec = pl.BlockSpec((full, local), lambda i, o: (0, 0))
    state_spec = pl.BlockSpec((heads, width, width), lambda i, o: (0, 0, 0))
    total_spec = pl.BlockSpec((heads, 128), lambda i, o: (0, 0))
    out_spec = pl.BlockSpec((block, local), lambda i, o: (i + skip, 0))
    held = len(parts) + 8
    return pl.pallas_call(
        functools.partial(
            project_kernel,
            pieces=len(parts),
            heads=heads,
            width=width,
            aliased=buffers is not None,
        ),
        grid_spec=pltpu.PrefetchScalarGridSpec(
            num_scalar_prefetch=1,
            grid=(chunk_rows // block,),
            in_specs=[pl.BlockSpec((heads, block), lambda i, o: (0, i + skip))]
            + [part_spec] * len(parts)
            + [weight_spec] * 4
            + [state_spec, total_spec]
            + ([] if buffers is None else [pl.BlockSpec(memory_space=pl.ANY)] * 4),
            out_specs=[out_spec] * 4 + [state_spec, total_spec],
        ),
        out_shape=[jax.ShapeDtypeStruct((rows, local), jnp.bfloat16)] * 4
        + [
            jax.ShapeDtypeStruct((heads, width, width), jnp.float32),
            jax.ShapeDtypeStruct((heads, 128), jnp.float32),
        ],
        input_output_aliases={} if buffers is None else {held + j: j for j in range(4)},
        cost_estimate=pl.CostEstimate(
            flops=8 * chunk_rows * full * local,
            bytes_accessed=8 * full * local + 8 * chunk_rows * local,
            transcendentals=0,
        ),
        name="project",
    )(order, decay_rows, *parts, *weights, before, total, *(buffers or ()))


def retain(decay_rows, queries, key_rows, values, initial, heads, width):
    rows, local = key_rows.shape
    block = block_of(rows, 256)
    token_spec = pl.BlockSpec((block, local), lambda i: (i, 0))
    return pl.pallas_call(
        functools.partial(retain_kernel, heads=heads, width=width),
        grid=(rows // block,),
        in_specs=[
            pl.BlockSpec((heads, block), lambda i: (0, i)),
            token_spec,
            token_spec,
            token_spec,
            pl.BlockSpec((heads, width, width), lambda i: (0, 0, 0)),
        ],
        out_specs=token_spec,
        out_shape=jax.ShapeDtypeStruct((rows, local), jnp.bfloat16),
        scratch_shapes=[pltpu.VMEM((heads, width, width), jnp.float32)],
        name="retain",
    )(decay_rows, queries, key_rows, values, initial)


def gated_norm(output, gate, gain):
    groups, rows, width = output.shape
    block = block_of(rows, 128)
    piece = pl.BlockSpec((groups, block, width), lambda i: (0, i, 0))
    return pl.pallas_call(
        norm_kernel,
        grid=(rows // block,),
        in_specs=[piece, piece, pl.BlockSpec((1, groups * width), lambda i: (0, 0))],
        out_specs=pl.BlockSpec((block, groups * width), lambda i: (i, 0)),
        out_shape=jax.ShapeDtypeStruct((rows, groups * width), jnp.bfloat16),
        name="gated_norm",
    )(output, gate, gain.reshape(1, -1))


def carried_in(state, total, axis, count):
    decay = jnp.exp(total[:, 0])
    sent = state.astype(jnp.bfloat16)
    incoming = None
    for hop in range(count - 1, 0, -1):
        moves = [(i, i + hop) for i in range(count - hop)]
        arrived = lax.ppermute(sent, axis, moves).astype(jnp.float32)
        if incoming is not None:
            factor = lax.ppermute(decay, axis, moves)
            arrived = arrived + factor[:, None, None] * incoming
        incoming = arrived
    return jnp.zeros_like(state) if incoming is None else incoming


def body(seq_count, mp_count, tokens, w_query, w_key, w_value, w_gate, decay_exponent, forget, norm_gain):
    seq_rows = tokens.shape[0]
    local_width = w_query.shape[1]
    heads = decay_exponent.shape[0]
    width = local_width // heads
    rate = jnp.log1p(-jnp.exp2(-decay_exponent.astype(jnp.float32)))
    decay_rows = rate[:, None] - forget.T

    def exchange(source):
        pieces = source.reshape(mp_count, seq_rows // mp_count, local_width)
        return lax.all_to_all(pieces, "mp", split_axis=0, concat_axis=0, tiled=True)

    place = lax.axis_index("mp")
    cores = 2 if mp_count % 2 == 0 else 1
    chips = mp_count // cores
    ways = [[(i, (i + cores * d) % mp_count) for i in range(mp_count)] for d in range(1, chips)]
    swap = [(i, i ^ 1) for i in range(mp_count)]
    chunk_count = CHUNKS if seq_rows % (CHUNKS * 8 * mp_count) == 0 else 1
    chunk_rows = seq_rows // chunk_count
    own = [tokens[c * chunk_rows : (c + 1) * chunk_rows] for c in range(chunk_count)]
    arrived = [[lax.ppermute(o, "mp", way) for way in ways] for o in own]
    near = [place] + [(place - cores * d) % mp_count for d in range(1, chips)]
    order = jnp.stack(near + ([n ^ 1 for n in near] if cores == 2 else [])).astype(jnp.int32)
    state = jnp.zeros((heads, width, width), jnp.float32)
    total = jnp.zeros((heads, 128), jnp.float32)
    weights = (w_gate, w_key, w_value, w_query)
    buffers = None
    for c in range(chunk_count):
        if c:
            arrived[c], state = lax.optimization_barrier((arrived[c], state))
        direct = [own[c]] + arrived[c]
        swapped = [lax.ppermute(d, "mp", swap) for d in direct] if cores == 2 else []
        *buffers, state, total = project_chunk(
            order,
            decay_rows,
            direct + swapped,
            weights,
            state,
            total,
            buffers,
            c * chunk_rows,
            seq_rows,
            heads,
            width,
        )
    gate, key_rows, values, queries = buffers
    incoming = carried_in(state, total, "seq", seq_count)
    moved_gate = exchange(gate)
    output = retain(decay_rows, queries, key_rows, values, incoming, heads, width)
    moved_output = exchange(output)
    return gated_norm(moved_output, moved_gate, norm_gain)


def solution(mesh):
    placed = (
        P(("dp", "seq"), "mp"),
        P(None, "mp"),
        P(None, "mp"),
        P(None, "mp"),
        P(None, "mp"),
        P("mp"),
        P(("dp", "seq"), "mp"),
        P(),
    )
    return jax.shard_map(
        functools.partial(body, mesh.shape["seq"], mesh.shape["mp"]),
        mesh=mesh,
        in_specs=placed,
        out_specs=P(("dp", "seq", "mp"), None),
        check_vma=False,
    )
```

```python
import functools

import jax
import jax.numpy as jnp
from jax import lax
from jax.experimental import pallas as pl
from jax.experimental.pallas import tpu as pltpu
from jax.sharding import PartitionSpec as P

DH = 128
CHUNKS = 4


def block_of(rows, most):
    block = min(rows, most)
    while rows % block:
        block //= 2
    return block


def running_sum(decay_rows):
    width = decay_rows.shape[1]
    upto = (
        lax.broadcasted_iota(jnp.int32, (width, width), 0)
        <= lax.broadcasted_iota(jnp.int32, (width, width), 1)
    ).astype(jnp.float32)
    return jnp.dot(
        decay_rows, upto, precision=lax.Precision.HIGHEST, preferred_element_type=jnp.float32
    )


def next_state(state, key_blk, value_blk, column, last):
    scaled = (key_blk.astype(jnp.float32) * jnp.exp(last - column)).astype(jnp.bfloat16)
    return jnp.exp(last) * state + lax.dot_general(
        scaled, value_blk, (((0,), (0,)), ((), ())), preferred_element_type=jnp.float32
    )


def project_kernel(order_ref, decay_ref, *refs, pieces, heads, width, aliased):
    parts = refs[:pieces]
    weights = refs[pieces : pieces + 4]
    before_ref, total_before_ref = refs[pieces + 4 : pieces + 6]
    outs = refs[pieces + 6 + (4 if aliased else 0) :]
    gate_ref, key_ref, value_ref, query_ref, state_ref, total_ref = outs[:6]
    held, arrival = outs[6:10], outs[10]
    copies = [pltpu.make_async_copy(weights[j], held[j], arrival.at[j]) for j in range(4)]

    @pl.when(pl.program_id(0) == 0)
    def _():
        for j in (1, 2, 0, 3):
            copies[j].start()
        state_ref[...] = before_ref[...]
        total_ref[...] = total_before_ref[...]

    depth = parts[0].shape[1]

    def project(j):
        weight = held[j]

        @pl.when(pl.program_id(0) == 0)
        def _():
            copies[j].wait()

        acc = None
        for p in range(pieces):
            start = pl.multiple_of(order_ref[p] * depth, depth)
            one = jnp.dot(
                parts[p][...],
                weight[pl.ds(start, depth), :],
                preferred_element_type=jnp.float32,
            )
            acc = one if acc is None else acc + one
        return acc

    key_ref[...] = (project(1) * DH ** (-0.5)).astype(jnp.bfloat16)
    value_ref[...] = project(2).astype(jnp.bfloat16)
    gate_ref[...] = project(0).astype(jnp.bfloat16)
    query_ref[...] = project(3).astype(jnp.bfloat16)
    running = running_sum(decay_ref[...])
    columns = running.T
    last_at = running.shape[1] - 1
    for h in range(heads):
        at = slice(h * width, (h + 1) * width)
        last = running[h : h + 1, last_at:]
        state_ref[h] = next_state(
            state_ref[h], key_ref[:, at], value_ref[:, at], columns[:, h : h + 1], last
        )
    total_ref[...] += jnp.broadcast_to(running[:, last_at:], total_ref.shape)


def retain_kernel(
    decay_ref, query_ref, key_ref, value_ref, initial_ref, out_ref, state_ref, *, first, heads, width
):
    @pl.when(pl.program_id(0) == 0)
    def _():
        state_ref[...] = initial_ref[...]

    running = running_sum(decay_ref[...])[first : first + heads]
    columns = running.T
    size = running.shape[1]
    causal = lax.broadcasted_iota(jnp.int32, (size, size), 0) >= lax.broadcasted_iota(
        jnp.int32, (size, size), 1
    )
    for h in range(heads):
        at = slice(h * width, (h + 1) * width)
        row = running[h : h + 1, :]
        column = columns[:, h : h + 1]
        last = running[h : h + 1, size - 1 :]
        query = query_ref[:, at]
        key_blk = key_ref[:, at]
        value_blk = value_ref[:, at]
        mask = jnp.where(causal, jnp.exp(column - row), 0.0)
        scores = lax.dot_general(
            query, key_blk, (((1,), (1,)), ((), ())), preferred_element_type=jnp.float32
        )
        scores = (scores * mask).astype(jnp.bfloat16)
        state = state_ref[h]
        inner = jnp.dot(scores, value_blk, preferred_element_type=jnp.float32)
        carried = jnp.dot(query, state.astype(jnp.bfloat16), preferred_element_type=jnp.float32)
        out_ref[:, at] = (inner + jnp.exp(column) * carried).astype(jnp.bfloat16)
        state_ref[h] = next_state(state, key_blk, value_blk, column, last)


def norm_kernel(gain_ref, gate_ref, *refs):
    out_refs, result_ref = refs[:-1], refs[-1]
    groups, _, width = gate_ref.shape
    part = width // len(out_refs)
    squares = 0.0
    for out_ref in out_refs:
        for g in range(groups):
            out = out_ref[g].astype(jnp.float32)
            squares = squares + jnp.sum(out * out, axis=1, keepdims=True)
    rstd = lax.rsqrt(squares / (groups * width) + 1e-06)
    for p, out_ref in enumerate(out_refs):
        for g in range(groups):
            at = slice(g * width + p * part, g * width + (p + 1) * part)
            gate = gate_ref[g, :, p * part : (p + 1) * part].astype(jnp.float32)
            silu = gate * (1.0 / (1.0 + jnp.exp(-gate)))
            result_ref[:, at] = (
                silu * out_ref[g].astype(jnp.float32) * rstd * gain_ref[:, at]
            ).astype(jnp.bfloat16)


def project_chunk(order, decay_rows, parts, weights, before, total, buffers, first, rows, heads, width):
    chunk_rows, depth = parts[0].shape
    full, local = weights[0].shape
    block = block_of(chunk_rows, 256)
    skip = first // block
    part_spec = pl.BlockSpec((block, depth), lambda i, o: (i, 0))
    weight_spec = pl.BlockSpec(memory_space=pl.ANY)
    state_spec = pl.BlockSpec((heads, width, width), lambda i, o: (0, 0, 0))
    total_spec = pl.BlockSpec((heads, 128), lambda i, o: (0, 0))
    out_spec = pl.BlockSpec((block, local), lambda i, o: (i + skip, 0))
    held = len(parts) + 8
    return pl.pallas_call(
        functools.partial(
            project_kernel,
            pieces=len(parts),
            heads=heads,
            width=width,
            aliased=buffers is not None,
        ),
        grid_spec=pltpu.PrefetchScalarGridSpec(
            num_scalar_prefetch=1,
            grid=(chunk_rows // block,),
            in_specs=[pl.BlockSpec((heads, block), lambda i, o: (0, i + skip))]
            + [part_spec] * len(parts)
            + [weight_spec] * 4
            + [state_spec, total_spec]
            + ([] if buffers is None else [pl.BlockSpec(memory_space=pl.ANY)] * 4),
            out_specs=[out_spec] * 4 + [state_spec, total_spec],
            scratch_shapes=[pltpu.VMEM((full, local), jnp.bfloat16)] * 4
            + [pltpu.SemaphoreType.DMA((4,))],
        ),
        out_shape=[jax.ShapeDtypeStruct((rows, local), jnp.bfloat16)] * 4
        + [
            jax.ShapeDtypeStruct((heads, width, width), jnp.float32),
            jax.ShapeDtypeStruct((heads, 128), jnp.float32),
        ],
        input_output_aliases={} if buffers is None else {held + j: j for j in range(4)},
        cost_estimate=pl.CostEstimate(
            flops=8 * chunk_rows * full * local,
            bytes_accessed=8 * full * local + 8 * chunk_rows * local,
            transcendentals=0,
        ),
        name="project",
    )(order, decay_rows, *parts, *weights, before, total, *(buffers or ()))


def retain(decay_rows, queries, key_rows, values, initial, first, group, width):
    rows = key_rows.shape[0]
    heads = decay_rows.shape[0]
    block = block_of(rows, 256)
    at = first // group
    token_spec = pl.BlockSpec((block, group * width), lambda i: (i, at))
    return pl.pallas_call(
        functools.partial(retain_kernel, first=first, heads=group, width=width),
        grid=(rows // block,),
        in_specs=[
            pl.BlockSpec((heads, block), lambda i: (0, i)),
            token_spec,
            token_spec,
            token_spec,
            pl.BlockSpec((group, width, width), lambda i: (at, 0, 0)),
        ],
        out_specs=pl.BlockSpec((block, group * width), lambda i: (i, 0)),
        out_shape=jax.ShapeDtypeStruct((rows, group * width), jnp.bfloat16),
        scratch_shapes=[pltpu.VMEM((group, width, width), jnp.float32)],
        cost_estimate=pl.CostEstimate(
            flops=16 * rows * block * group * width, bytes_accessed=8 * rows * group * width, transcendentals=0
        ),
        name="retain",
    )(decay_rows, queries, key_rows, values, initial)


def gated_norm(outputs, gate, gain):
    groups, rows, width = gate.shape
    block = block_of(rows, 128)

    def piece(source):
        return pl.BlockSpec((groups, block, source.shape[2]), lambda i: (0, i, 0))

    return pl.pallas_call(
        norm_kernel,
        grid=(rows // block,),
        in_specs=[pl.BlockSpec((1, groups * width), lambda i: (0, 0)), piece(gate)]
        + [piece(o) for o in outputs],
        out_specs=pl.BlockSpec((block, groups * width), lambda i: (i, 0)),
        out_shape=jax.ShapeDtypeStruct((rows, groups * width), jnp.bfloat16),
        name="gated_norm",
    )(gain.reshape(1, -1), gate, *outputs)


def carried_in(state, total, axis, count):
    decay = jnp.exp(total[:, 0])
    sent = state.astype(jnp.bfloat16)
    incoming = None
    for hop in range(count - 1, 0, -1):
        moves = [(i, i + hop) for i in range(count - hop)]
        arrived = lax.ppermute(sent, axis, moves).astype(jnp.float32)
        if incoming is not None:
            factor = lax.ppermute(decay, axis, moves)
            arrived = arrived + factor[:, None, None] * incoming
        incoming = arrived
    return jnp.zeros_like(state) if incoming is None else incoming


def body(seq_count, mp_count, tokens, w_query, w_key, w_value, w_gate, decay_exponent, forget, norm_gain):
    seq_rows = tokens.shape[0]
    local_width = w_query.shape[1]
    heads = decay_exponent.shape[0]
    width = local_width // heads
    rate = jnp.log1p(-jnp.exp2(-decay_exponent.astype(jnp.float32)))
    decay_rows = rate[:, None] - forget.T

    def exchange(source):
        pieces = source.reshape(mp_count, seq_rows // mp_count, source.shape[1])
        return lax.all_to_all(pieces, "mp", split_axis=0, concat_axis=0, tiled=True)

    place = lax.axis_index("mp")
    cores = 2 if mp_count % 2 == 0 else 1
    chips = mp_count // cores
    ways = [[(i, (i + cores * d) % mp_count) for i in range(mp_count)] for d in range(1, chips)]
    swap = [(i, i ^ 1) for i in range(mp_count)]
    chunk_count = CHUNKS if seq_rows % (CHUNKS * 8 * mp_count) == 0 else 1
    chunk_rows = seq_rows // chunk_count
    own = [tokens[c * chunk_rows : (c + 1) * chunk_rows] for c in range(chunk_count)]
    arrived = [[lax.ppermute(o, "mp", way) for way in ways] for o in own]
    near = [place] + [(place - cores * d) % mp_count for d in range(1, chips)]
    order = jnp.stack(near + ([n ^ 1 for n in near] if cores == 2 else [])).astype(jnp.int32)
    state = jnp.zeros((heads, width, width), jnp.float32)
    total = jnp.zeros((heads, 128), jnp.float32)
    weights = (w_gate, w_key, w_value, w_query)
    buffers = None
    for c in range(chunk_count):
        if c:
            arrived[c], state = lax.optimization_barrier((arrived[c], state))
        direct = [own[c]] + arrived[c]
        swapped = [lax.ppermute(d, "mp", swap) for d in direct] if cores == 2 else []
        *buffers, state, total = project_chunk(
            order,
            decay_rows,
            direct + swapped,
            weights,
            state,
            total,
            buffers,
            c * chunk_rows,
            seq_rows,
            heads,
            width,
        )
    gate, key_rows, values, queries = buffers
    incoming = carried_in(state, total, "seq", seq_count)
    moved_gate = exchange(gate)
    group = heads
    moved = [
        exchange(retain(decay_rows, queries, key_rows, values, incoming, first, group, width))
        for first in range(0, heads, group)
    ]
    return gated_norm(moved, moved_gate, norm_gain)


def solution(mesh):
    placed = (
        P(("dp", "seq"), "mp"),
        P(None, "mp"),
        P(None, "mp"),
        P(None, "mp"),
        P(None, "mp"),
        P("mp"),
        P(("dp", "seq"), "mp"),
        P(),
    )
    return jax.shard_map(
        functools.partial(body, mesh.shape["seq"], mesh.shape["mp"]),
        mesh=mesh,
        in_specs=placed,
        out_specs=P(("dp", "seq", "mp"), None),
        check_vma=False,
    )
```
